256 devices in a mesh: terms: 256 (over z, y, x, core).
Axes of the slice: x: 4, y: 4, z: 8, core: 2. Of those that a mesh axis runs over, the one named last changes fastest.
Arguments:
- psi_init: float32 [256, 4, 4, 256], replicated
- left_env: bfloat16 [1536, 256, 256], P('terms')
- op_pair: bfloat16 [1536, 16, 16], P('terms')
- right_env: bfloat16 [1536, 256, 256], P('terms')
Outputs:
- output 1: float32 [7, 256, 4, 4, 256], P(None, 'terms')
- output 2: float32 [6], replicated
- output 3: float32 [6], replicated
All inputs are finite; a program needn't handle non-finite values.
Results may differ from the reference program's by a relative error of at most 0.0176077.
Values are sent between devices in bfloat16 or wider.
A program may use at most 768 MiB of HBM per device.

```python
import jax
import jax.numpy as jnp
from jax import lax

BOND = 256
PHYS = 4
TERMS = 1536
KRYLOV_STEPS = 6


def symmetric_stack(key_in, count, size):
    gauss_draws = jax.random.normal(key_in, (count, size, size), jnp.float32)
    return (gauss_draws + jnp.swapaxes(gauss_draws, 1, 2)) * (0.5 * (2.0 * size) ** -0.5)


def setup_inputs(seed: int = 0) -> dict:
    root_key = jax.random.key(seed)
    key_psi, key_left, key_pair, key_right, key_shift = jax.random.split(root_key, 5)
    pair_dim = PHYS * PHYS
    shifts = 0.5 * jax.random.normal(key_shift, (3, TERMS), jnp.float32)
    eye_bond = jnp.eye(BOND, dtype=jnp.float32)
    eye_pair = jnp.eye(pair_dim, dtype=jnp.float32)
    term_scale = 2.0 * TERMS ** -0.5
    psi_init = jax.random.normal(key_psi, (BOND, PHYS, PHYS, BOND), jnp.float32)
    left_env = term_scale * (symmetric_stack(key_left, TERMS, BOND) + shifts[0][:, None, None] * eye_bond)
    op_pair = symmetric_stack(key_pair, TERMS, pair_dim) + shifts[1][:, None, None] * eye_pair
    right_env = symmetric_stack(key_right, TERMS, BOND) + shifts[2][:, None, None] * eye_bond
    return {'psi_init': psi_init, 'left_env': left_env.astype(jnp.bfloat16), 'op_pair': op_pair.astype(jnp.bfloat16), 'right_env': right_env.astype(jnp.bfloat16)}


def reference(psi_init, left_env, op_pair, right_env):
    pair_dim = PHYS * PHYS
    elem_count = BOND * pair_dim * BOND

    def apply_terms(vector):
        vector_low = vector.astype(jnp.bfloat16).reshape(BOND * pair_dim, BOND)

        def one_term(sigma_sum, term_mats):
            left_mat, pair_mat, right_mat = term_mats
            y_part = jnp.dot(vector_low, right_mat.T, preferred_element_type=jnp.float32)
            y_part = y_part.astype(jnp.bfloat16).reshape(BOND, pair_dim, BOND)
            z_part = jnp.einsum('qp,apb->aqb', pair_mat.astype(jnp.float32), y_part.astype(jnp.float32))
            z_part = z_part.astype(jnp.bfloat16).reshape(BOND, pair_dim * BOND)
            term_out = jnp.dot(left_mat, z_part, preferred_element_type=jnp.float32)
            return sigma_sum + term_out.reshape(BOND, pair_dim, BOND), None

        sigma_sum, _ = lax.scan(one_term, jnp.zeros((BOND, pair_dim, BOND), jnp.float32), (left_env, op_pair, right_env))
        return sigma_sum

    vector = psi_init.reshape(BOND, pair_dim, BOND)
    vector = vector / jnp.sqrt(jnp.sum(vector * vector) / elem_count)
    vectors = [vector]
    alphas = []
    betas = []
    prev_vector = vector
    for step_idx in range(KRYLOV_STEPS):
        sigma_sum = apply_terms(vector)
        alpha_val = jnp.sum(sigma_sum * vector) / elem_count
        residual = sigma_sum - alpha_val * vector
        if step_idx > 0:
            residual = residual - betas[-1] * prev_vector
        beta_val = jnp.sqrt(jnp.sum(residual * residual) / elem_count)
        prev_vector = vector
        vector = residual / beta_val
        vectors.append(vector)
        alphas.append(alpha_val)
        betas.append(beta_val)
    krylov_vectors = jnp.stack(vectors).reshape(KRYLOV_STEPS + 1, BOND, PHYS, PHYS, BOND)
    return krylov_vectors, jnp.stack(alphas), jnp.stack(betas)
```

```python
import functools
import jax
import jax.numpy as jnp
from jax import lax
from jax.experimental import pallas as pl
from jax.experimental.pallas import tpu as pltpu
from jax.sharding import PartitionSpec as P

STEPS = 6
Z, Y, X, C = 8, 4, 4, 2
BOND, PAIR = 256, 16
OWN = 6
MEMB = X * C
GROUP = OWN * MEMB
SLAB = BOND // MEMB
COUNT = BOND * PAIR * BOND
F32, BF16 = jnp.float32, jnp.bfloat16
MESH = pl.DeviceIdType.MESH


def kernel(psi, left, wide, right, out, alphas, betas,
           lst, wall, rall, kron, u, vb, v, s, acc, yrecv, zsend, zrecv,
           loc_sem, l_send, l_recv, r_send, r_recv, rx_send, rs_send, rs_recv,
           ag_send, ag_recv, rl_send, rl_recv, d_send, d_recv):
    me = lax.axis_index("terms")
    c = lax.rem(me, C)
    x = lax.rem(me // C, X)
    y = lax.rem(me // (C * X), Y)
    z = me // (C * X * Y)
    mem = me % MEMB

    def dev(zz, yy, xx, cc):
        return (((zz * Y + yy) * X + xx) * C + cc,)

    def up(pos, step, size):
        return lax.rem(pos + step, size)

    def send(src, dst, ssem, rsem, to):
        copy = pltpu.make_async_remote_copy(src, dst, ssem, rsem, device_id=to, device_id_type=MESH)
        copy.start()
        return copy

    sib = dev(z, y, x, 1 - c)
    barrier = pltpu.get_barrier_semaphore()
    peers = [dev(up(z, d, Z), y, x, c) for d in range(1, Z)]
    peers += [dev(z, up(y, d, Y), x, c) for d in range(1, Y)]
    peers += [dev(z, y, up(x, d, X), cc) for d in range(1, X) for cc in range(C)]
    peers += [sib]
    for peer in peers:
        pl.semaphore_signal(barrier, inc=1, device_id=peer, device_id_type=MESH)

    own = pl.ds(OWN * mem, OWN)
    local = [pltpu.make_async_copy(psi, v.at[0], loc_sem.at[0]),
             pltpu.make_async_copy(left.at[:, pl.ds(pl.multiple_of(SLAB * mem, SLAB), SLAB)], lst.at[own], loc_sem.at[1]),
             pltpu.make_async_copy(right, rall.at[own], loc_sem.at[2]),
             pltpu.make_async_copy(wide, wall.at[own], loc_sem.at[3])]
    for copy in local:
        copy.start()
    pl.semaphore_wait(barrier, len(peers))

    half = OWN // 2

    def rblk(m, h):
        return rall.at[pl.ds(OWN * m + half * h, half)]

    xp, xm = up(x, 1, X), up(x, X - 1, X)
    early = []
    for d in range(MEMB - 1):
        to = lax.rem(mem + 1 + d, MEMB)
        early.append(send(left.at[:, pl.ds(pl.multiple_of(SLAB * to, SLAB), SLAB)], lst.at[own],
                          l_send.at[0, d], l_recv.at[0, d], dev(z, y, to // C, to % C)))
        early.append(send(wide, wall.at[own], l_send.at[1, d], l_recv.at[1, d], dev(z, y, to // C, to % C)))
    rp, rm, rd = [], [], []
    for h in (0, 1):
        src = right.at[pl.ds(half * h, half)]
        rp.append(send(src, rblk(mem, h), r_send.at[0, h], r_recv.at[0, h], dev(z, y, xp, c)))
        g = 1 - h
        src = right.at[pl.ds(half * g, half)]
        rm.append(send(src, rblk(mem, g), r_send.at[1, g], r_recv.at[1, g], dev(z, y, xm, c)))
    for h in (0, 1):
        rd.append(send(right.at[pl.ds(half * h, half)], rblk(mem, h), r_send.at[2, h], r_recv.at[2, h], sib))

    zero = jnp.zeros((64, BOND), F32)

    def clear(i, _):
        v[1, i // 4, pl.ds(pl.multiple_of((i % 4) * 64, 64), 64)] = zero
        return 0

    lax.fori_loop(0, 64, clear, 0)
    for copy in local:
        copy.wait()

    def vsl(i):
        return i // 4, pl.ds(pl.multiple_of((i % 4) * 64, 64), 64)

    def fold(t):
        return jnp.sum(t.reshape(8, 8, BOND), axis=0)

    def total(t):
        return jnp.sum(jnp.sum(t, axis=0, keepdims=True), axis=1, keepdims=True)

    def sq(i, t):
        q, r = vsl(i)
        blk = v[0, q, r]
        return t + fold(blk * blk)

    nrm = jnp.sqrt(total(lax.fori_loop(0, 64, sq, jnp.zeros((8, BOND), F32))) / COUNT)
    inv0 = 1.0 / nrm

    def scale0(i, _):
        q, r = vsl(i)
        blk = v[0, q, r] * inv0
        v[0, q, r] = blk
        vb[q, r] = blk.astype(BF16)
        return 0

    lax.fori_loop(0, 64, scale0, 0)

    def emit(row, slot):
        def one(q, _):
            out[row, pl.ds(q, 1)] = v[slot, q, pl.ds(me, 1)]
            return 0
        lax.fori_loop(0, PAIR, one, 0)

    emit(0, 0)
    for copy in early:
        copy.wait_recv()
    lane = lax.broadcasted_iota(jnp.int32, (16, 256), 1) % 16
    rowi = lax.broadcasted_iota(jnp.int32, (16, 256), 0)
    diag = lane == rowi

    def build(k, _):
        wk = wall[k].astype(F32)
        for q in range(PAIR):
            blk = jnp.where(diag, jnp.broadcast_to(wk[q:q + 1], (16, 256)), 0.0)
            kron[k, 16 * q:16 * q + 16] = blk.astype(BF16)
        return 0

    lax.fori_loop(0, GROUP, build, 0)

    mp, mm, m2 = C * xp + c, C * xm + c, C * up(x, 2, X) + c
    rp[0].wait_recv()
    fw = [send(rblk(mm, 0), rblk(mm, 0), rx_send.at[0], r_recv.at[3, 0], dev(z, y, xp, c)),
          send(rblk(mm, 0), rblk(mm, 0), rx_send.at[2], r_recv.at[4, 0], sib)]
    rm[0].wait_recv()
    fw += [send(rblk(mp, 1), rblk(mp, 1), rx_send.at[1], r_recv.at[3, 1], dev(z, y, xm, c)),
           send(rblk(mp, 1), rblk(mp, 1), rx_send.at[3], r_recv.at[4, 1], sib)]
    rp[1].wait_recv()
    fw += [send(rblk(mm, 1), rblk(mm, 1), rx_send.at[4], r_recv.at[5, 0], sib)]
    rm[1].wait_recv()
    fw += [send(rblk(mp, 0), rblk(mp, 0), rx_send.at[5], r_recv.at[5, 1], sib)]
    fw[0].wait_recv()
    fw += [send(rblk(m2, 0), rblk(m2, 0), rx_send.at[6], r_recv.at[6, 0], sib)]
    fw[2].wait_recv()
    fw += [send(rblk(m2, 1), rblk(m2, 1), rx_send.at[7], r_recv.at[6, 1], sib)]
    for copy in rd:
        copy.wait_recv()
    for i in (1, 3, 4, 5, 6, 7):
        fw[i].wait_recv()
    for copy in early + rp + rm + rd + fw:
        copy.wait_send()

    def matvec():
        def one(p, _):
            w = jnp.dot(lst[...].reshape(GROUP * SLAB, BOND), vb[p], preferred_element_type=F32)
            u[p] = w.astype(BF16).reshape(GROUP, SLAB, BOND)
            return 0
        lax.fori_loop(0, PAIR, one, 0)
        acc[...] = jnp.zeros_like(acc)
        UN = 4

        def terms(kk, _):
            res = None
            for i in range(UN):
                k = kk * UN + i
                zs = []
                for t in range(2):
                    blk = u[:, k, 16 * t:16 * t + 16].reshape(256, BOND)
                    zs.append(jnp.dot(kron[k], blk, preferred_element_type=F32).astype(BF16))
                o = jnp.dot(jnp.concatenate(zs, axis=0), rall[k], preferred_element_type=F32)
                res = o if res is None else res + o
            acc[...] += res.reshape(2, PAIR, 2, 8, BOND)
            return 0
        lax.fori_loop(0, GROUP // UN, terms, 0)

    def step(j, beta_prev):
        par = lax.rem(j, 2)
        matvec()
        ry = []
        for d in range(1, Y):
            yt = up(y, d, Y)
            ry.append(send(acc.at[yt // 2, :, yt % 2], yrecv.at[d - 1], rs_send.at[d - 1], rs_recv.at[d - 1], dev(z, yt, x, c)))
        for copy in ry:
            copy.wait_recv()
        ysum = acc[y // 2, :, y % 2] + yrecv[0] + yrecv[1] + yrecv[2]
        zsend[...] = ysum.reshape(Z, 2, 8, BOND)
        rz = []
        for d in range(1, Z):
            zt = up(z, d, Z)
            rz.append(send(zsend.at[zt], zrecv.at[d - 1], rs_send.at[2 + d], rs_recv.at[2 + d], dev(zt, y, x, c)))
        for copy in rz:
            copy.wait_recv()
        zsum = zsend[z]
        for d in range(Z - 1):
            zsum = zsum + zrecv[d]
        s[par, pl.ds(2 * z, 2), x, c, y] = zsum

        sent = list(ry) + list(rz)
        ch = s.at[par, pl.ds(2 * z, 2), x, c, y]
        gz = [send(ch, ch, ag_send.at[par, d - 1], ag_recv.at[par, d - 1], dev(up(z, d, Z), y, x, c)) for d in range(1, Z)]
        for copy in gz:
            copy.wait_recv()
        sent += gz
        lo, hi = pl.ds(0, 128), pl.ds(128, 128)
        q0, q1, qa = pl.ds(0, 8), pl.ds(8, 8), pl.ds(0, 16)
        yp, ym, y2 = up(y, 1, Y), up(y, Y - 1, Y), up(y, 2, Y)
        x2 = up(x, 2, X)
        tyP, tyM = dev(z, yp, x, c), dev(z, ym, x, c)
        txP, txM = dev(z, y, xp, c), dev(z, y, xm, c)

        def a2(yy, q):
            return s.at[par, q, x, c, yy, :, lo]

        def b2(xx, q):
            return s.at[par, q, xx, c, y, :, hi]

        def a3(xx, q):
            return s.at[par, q, xx, c, :, :, lo]

        def b3(yy, q):
            return s.at[par, q, :, c, yy, :, hi]

        def go(ref, i, to):
            copy = send(ref, ref, rl_send.at[par, i], rl_recv.at[par, i], to)
            sent.append(copy)
            return copy

        def ring2(fa, fb, base):
            (f, own_, p_, m_, tP, tM), (g, gown, gp_, gm_, sP, sM) = fa, fb
            k = [go(f(own_, qa), base, tP), go(f(own_, qa), base + 1, tM),
                 go(g(gown, qa), base + 2, sP), go(g(gown, qa), base + 3, sM)]
            k[0].wait_recv()
            k.append(go(f(m_, q0), base + 4, tP))
            k[1].wait_recv()
            k.append(go(f(p_, q1), base + 5, tM))
            k[2].wait_recv()
            k.append(go(g(gm_, q0), base + 6, sP))
            k[3].wait_recv()
            k.append(go(g(gp_, q1), base + 7, sM))
            return k[4:]

        for copy in ring2((a2, y, yp, ym, tyP, tyM), (b2, x, xp, xm, txP, txM), 0):
            copy.wait_recv()
        dd = []

        def cross(ref, i):
            copy = send(ref, ref, d_send.at[par, i], d_recv.at[par, i], sib)
            sent.append(copy)
            dd.append(copy)

        k3 = ring2((a3, x, xp, xm, txP, txM), (b3, y, yp, ym, tyP, tyM), 8)
        cross(a3(x, qa), 0)
        cross(b3(y, qa), 1)
        cross(a3(xm, qa), 2)
        cross(a3(xp, qa), 3)
        cross(b3(ym, qa), 4)
        cross(b3(yp, qa), 5)
        k3[0].wait_recv()
        k3[1].wait_recv()
        cross(a3(x2, qa), 6)
        k3[2].wait_recv()
        k3[3].wait_recv()
        cross(b3(y2, qa), 7)
        for copy in dd:
            copy.wait_recv()
        for copy in sent:
            copy.wait_send()

        cur, prev = lax.rem(j, 2), lax.rem(j + 1, 2)

        def sload(i):
            return s[par, i // 4, i % 4].reshape(64, BOND)

        def dot_sv(i, t):
            q, r = vsl(i)
            return t + fold(sload(i) * v[cur, q, r])

        alpha = total(lax.fori_loop(0, 64, dot_sv, jnp.zeros((8, BOND), F32))) / COUNT

        def resid(i, t):
            q, r = vsl(i)
            w = sload(i) - alpha * v[cur, q, r] - beta_prev * v[prev, q, r]
            v[prev, q, r] = w
            return t + fold(w * w)

        beta = jnp.sqrt(total(lax.fori_loop(0, 64, resid, jnp.zeros((8, BOND), F32))) / COUNT)
        inv = 1.0 / beta

        def scale(i, _):
            q, r = vsl(i)
            w = v[prev, q, r] * inv
            v[prev, q, r] = w
            vb[q, r] = w.astype(BF16)
            return 0

        lax.fori_loop(0, 64, scale, 0)
        emit(j + 1, prev)
        alphas[j] = alpha[0, 0]
        betas[j] = beta[0, 0]
        return beta

    lax.fori_loop(0, STEPS, step, jnp.zeros((1, 1), F32))


def solution(mesh):
    def local_run(psi_init, left_env, op_pair, right_env):
        psi_t = jnp.transpose(psi_init.reshape(BOND, PAIR, BOND), (1, 0, 2))
        wide = jnp.repeat(op_pair, 16, axis=2)
        dma = pltpu.SemaphoreType.DMA
        any_ = pl.BlockSpec(memory_space=pl.ANY)
        out, al, be = pl.pallas_call(
            kernel,
            out_shape=(jax.ShapeDtypeStruct((STEPS + 1, PAIR, BOND), F32),
                       jax.ShapeDtypeStruct((STEPS,), F32),
                       jax.ShapeDtypeStruct((STEPS,), F32)),
            in_specs=[any_] * 4,
            out_specs=(pl.BlockSpec(memory_space=pltpu.VMEM),
                       pl.BlockSpec(memory_space=pltpu.SMEM),
                       pl.BlockSpec(memory_space=pltpu.SMEM)),
            scratch_shapes=[
                pltpu.VMEM((GROUP, SLAB, BOND), BF16),
                pltpu.VMEM((GROUP, PAIR, 256), BF16),
                pltpu.VMEM((GROUP, BOND, BOND), BF16),
                pltpu.VMEM((GROUP, 256, 256), BF16),
                pltpu.VMEM((PAIR, GROUP, SLAB, BOND), BF16),
                pltpu.VMEM((PAIR, BOND, BOND), BF16),
                pltpu.VMEM((2, PAIR, BOND, BOND), F32),
                pltpu.VMEM((2, PAIR, X, C, Y, 8, BOND), F32),
                pltpu.VMEM((2, PAIR, 2, 8, BOND), F32),
                pltpu.VMEM((Y - 1, PAIR, 8, BOND), F32),
                pltpu.VMEM((Z, 2, 8, BOND), F32),
                pltpu.VMEM((Z - 1, 2, 8, BOND), F32),
                dma((4,)), dma((2, 7)), dma((2, 7)),
                dma((3, 2)), dma((7, 2)), dma((8,)),
                dma((10,)), dma((10,)),
                dma((2, 7)), dma((2, 7)),
                dma((2, 16)), dma((2, 16)),
                dma((2, 8)), dma((2, 8)),
            ],
            compiler_params=pltpu.CompilerParams(
                collective_id=0, has_side_effects=True, vmem_limit_bytes=66 * 1000 * 1000),
        )(psi_t, left_env, wide, right_env)
        return out.reshape(STEPS + 1, 1, 4, 4, BOND), al, be

    return jax.shard_map(local_run, mesh=mesh, in_specs=(P(), P("terms"), P("terms"), P("terms")),
                         out_specs=(P(None, "terms"), P(), P()), check_vma=False)
```

```python
import jax
import jax.numpy as jnp
from jax import lax
from jax.experimental import pallas as pl
from jax.experimental.pallas import tpu as pltpu
from jax.sharding import PartitionSpec as P

STEPS = 6
Z, Y, X, C = 8, 4, 4, 2
BOND, PAIR = 256, 16
OWN = 6
MEMB = X * C
GROUP = OWN * MEMB
SLAB = BOND // MEMB
PART = 3
PT = OWN // PART
COUNT = BOND * PAIR * BOND
UNROLL = 24
QY = PAIR // Y
DIRECT2 = ("2",)
F32, BF16 = jnp.float32, jnp.bfloat16
MESH = pl.DeviceIdType.MESH


class Span:
    def __init__(self):
        self.open = None

    def __call__(self, name):
        if self.open is not None:
            self.open.__exit__(None, None, None)
        self.open = None
        if name:
            self.open = jax.named_scope(name)
            self.open.__enter__()


def kernel(psi, left, ops, right, out, scalars,
           lst, wall, wide, rall, kron, u, vb, v, s, acc, yrecv, zsend, zrecv, ssend, srecv, ay, az, am, rown, rsib, rrecv,
           loc_sem, l_send, l_recv, r_send, r_recv, y_send, y_recv, z_send, z_recv,
           gz_send, gz_recv, gr_send, gr_recv, c_send, c_recv, a_send, a_recv, b_send, b_recv, row_send, row_recv):
    me = lax.axis_index("terms")
    sp = Span()
    c = lax.rem(me, C)
    x = lax.rem(me // C, X)
    y = lax.rem(me // (C * X), Y)
    z = me // (C * X * Y)
    mem = lax.rem(me, MEMB)

    def dev(zz, yy, xx, cc):
        return (((zz * Y + yy) * X + xx) * C + cc,)

    def up(pos, step, size):
        return lax.rem(pos + step, size)

    def send(src, dst, ssem, rsem, to):
        copy = pltpu.make_async_remote_copy(src, dst, ssem, rsem, device_id=to, device_id_type=MESH)
        copy.start()
        return copy

    xp, xm, x2 = up(x, 1, X), up(x, X - 1, X), up(x, 2, X)
    yp, ym, y2 = up(y, 1, Y), up(y, Y - 1, Y), up(y, 2, Y)
    sib = dev(z, y, x, 1 - c)
    txp, txm = dev(z, y, xp, c), dev(z, y, xm, c)
    typ, tym = dev(z, yp, x, c), dev(z, ym, x, c)

    sp("entry")
    barrier = pltpu.get_barrier_semaphore()
    peers = [dev(up(z, d, Z), y, x, c) for d in range(1, Z)]
    peers += [dev(z, up(y, d, Y), x, c) for d in range(1, Y)]
    peers += [dev(z, y, up(x, d, X), cc) for d in range(1, X) for cc in range(C)]
    peers += [sib]
    for peer in peers:
        pl.semaphore_signal(barrier, inc=1, device_id=peer, device_id_type=MESH)
    own = pl.ds(OWN * mem, OWN)
    local = [pltpu.make_async_copy(psi.at[:, c, :, p // 4, p % 4, :], v.at[0, p], loc_sem.at[4 + p]) for p in range(PAIR)]
    local = local[::-1] + [
             pltpu.make_async_copy(left.at[:, pl.ds(pl.multiple_of(SLAB * mem, SLAB), SLAB)], lst.at[own], loc_sem.at[1]),
             pltpu.make_async_copy(right, rall.at[own], loc_sem.at[2]),
             pltpu.make_async_copy(ops, wall.at[own], loc_sem.at[3])]
    for copy in local:
        copy.start()
    pl.semaphore_wait(barrier, len(peers))

    early = []
    for d in range(MEMB - 1):
        to = lax.rem(mem + 1 + d, MEMB)
        early.append(send(left.at[:, pl.ds(pl.multiple_of(SLAB * to, SLAB), SLAB)], lst.at[own],
                          l_send.at[0, d], l_recv.at[0, d], dev(z, y, to // C, lax.rem(to, C))))
        early.append(send(ops, wall.at[own], l_send.at[1, d], l_recv.at[1, d],
                          dev(z, y, to // C, lax.rem(to, C))))

    def rpart(m, h):
        return rall.at[pl.ds(OWN * m + PT * h, PT)]

    pend = []
    H = BOND // 2

    def quads(ref, k0):
        return ref.at[pl.ds(k0, PT), pl.ds(0, H)], ref.at[pl.ds(k0, PT), pl.ds(H, H), pl.ds(H, H)]

    def rsend(src, dst, i, kind, to):
        copy = send(src, dst, r_send.at[i, kind], r_recv.at[i, kind], to)
        pend.append(copy)
        return copy

    def qsend(src, k0, m, h, i, to, kinds=(0, 1)):
        a, b = quads(src, k0), quads(rall, OWN * m + PT * h)
        return [rsend(a[kind], b[kind], i, kind, to) for kind in kinds]

    def mirror(m, h):
        for i in range(PT):
            k = OWN * m + PT * h + i
            rall[k, H:, :H] = rall[k, :H, H:].T

    def rpart(m, h):
        return rall.at[pl.ds(OWN * m + PT * h, PT)]

    from_xm, from_xp, from_sib = {}, {}, {}
    for h in range(PART):
        g = PART - 1 - h
        from_xm[h] = qsend(right, PT * h, mem, h, h, txp)
        from_xp[g] = qsend(right, PT * g, mem, g, PART + g, txm)
    for h in range(PART):
        from_sib[h] = rsend(right.at[pl.ds(PT * h, PT)], rpart(mem, h), 2 * PART + h, 0, sib)

    def chunk(i):
        return i // 2, pl.ds((i % 2) * 2, 2)

    NCH = 2 * PAIR

    def vload(slot, i):
        q, xx = chunk(i)
        return v[slot, q, xx].reshape(64, BOND)

    def vstore(slot, i, val):
        q, xx = chunk(i)
        v[slot, q, xx] = val.reshape(2, SLAB, BOND)

    def sload(par, i):
        q, xx = chunk(i)
        return s[par, q, xx].reshape(64, BOND)

    def fold(t):
        return jnp.sum(t.reshape(8, 8, BOND), axis=0)

    def both(part, i):
        tile = part[:, :128] + part[:, 128:]
        ssend[i] = tile
        copy = send(ssend.at[i], srecv.at[i], c_send.at[i], c_recv.at[i], sib)
        copy.wait()
        t = tile + srecv[i]
        return jnp.sum(jnp.sum(t, axis=0, keepdims=True), axis=1, keepdims=True)

    inhalf = me // (BOND // X)

    other = me + 1 - 2 * c
    QG = PAIR // 4

    def vbcopy(g):
        ref = vb.at[pl.ds(QG * g, QG), :, c]
        return pltpu.make_async_remote_copy(ref, ref, b_send.at[g], b_recv.at[g], device_id=sib, device_id_type=MESH)

    def finish(slot, inv, row):
        copies = []
        for g in range(4):
            def one(i, _):
                w = vload(slot, i) * inv
                vstore(slot, i, w)
                q, xx = chunk(i)
                vb[q, xx, c] = w.astype(BF16).reshape(2, SLAB, BOND)
                return 0
            lax.fori_loop(NCH // 4 * g, NCH // 4 * (g + 1), one, 0, unroll=2)
            copies.append(vbcopy(g))
            copies[-1].start()

        def pick(q, _):
            rown[row, pl.ds(q, 1)] = v[slot, q, inhalf, pl.ds(lax.rem(me, SLAB), 1)]
            rsib[row, pl.ds(q, 1)] = v[slot, q, inhalf, pl.ds(lax.rem(other, SLAB), 1)]
            return 0

        lax.fori_loop(0, PAIR, pick, 0, unroll=4)
        copies.append(send(rsib.at[row], rrecv.at[row], row_send.at[0], row_recv.at[0], sib))
        return copies

    def first(copies):
        rows = lst[...].reshape(GROUP * SLAB, BOND)
        for g in range(4):
            copies[g].wait_recv()
            for p in range(QG * g, QG * g + QG):
                w = jnp.dot(rows, vb[p].reshape(BOND, BOND), preferred_element_type=F32)
                u[p] = w.astype(BF16).reshape(GROUP, SLAB, BOND)
        settle(copies, 4)

    def settle(copies, n):
        for copy in copies[n:]:
            copy.wait_recv()
        for copy in copies:
            copy.wait_send()

    sp("init")
    for copy in local:
        copy.wait()

    def sq(i, t):
        blk = vload(0, i)
        return t + fold(blk * blk)

    def clear(i, _):
        vstore(1, i, jnp.zeros((64, BOND), F32))
        return 0

    lax.fori_loop(0, NCH, clear, 0)
    part = lax.fori_loop(0, NCH, sq, jnp.zeros((8, BOND), F32), unroll=2)
    nrm = jnp.sqrt(both(part, 0) / COUNT)
    begun = finish(0, 1.0 / nrm, 0)

    sp("waitL")
    for copy in early:
        copy.wait_recv()
    sp("build")
    lane = lax.broadcasted_iota(jnp.int32, (16, 256), 1) % 16
    rowi = lax.broadcasted_iota(jnp.int32, (16, 256), 0)
    diag = lane == rowi

    spread = lax.broadcasted_iota(jnp.int32, (PAIR, 256), 0) == lax.broadcasted_iota(jnp.int32, (PAIR, 256), 1) // 16
    rows = jnp.dot(wall[...].reshape(GROUP * PAIR, PAIR), spread.astype(F32).astype(BF16), preferred_element_type=F32)
    wide[...] = rows.reshape(GROUP, PAIR, 256)

    def build(k, _):
        wk = wide[k]
        for q in range(PAIR):
            blk = jnp.where(diag, jnp.broadcast_to(wk[q:q + 1], (16, 256)), 0.0)
            kron[k, 16 * q:16 * q + 16] = blk.astype(BF16)
        return 0

    lax.fori_loop(0, GROUP, build, 0)

    def rest(ks, ts):
        res = None
        for k in ks:
            zs = []
            for t in ts:
                blk = u[:, k, 16 * t:16 * t + 16].reshape(256, BOND)
                zs.append(jnp.dot(kron[k], blk, preferred_element_type=F32).astype(BF16))
            zk = zs[0] if len(zs) == 1 else jnp.concatenate(zs, axis=0)
            o = jnp.dot(zk, rall[k], preferred_element_type=F32)
            res = o if res is None else res + o
        for i, t in enumerate(ts):
            acc[t] += res[256 * i:256 * i + 256].reshape(Y, QY, 16, BOND)

    def ycopy(t, d):
        yt = up(y, d, Y)
        return pltpu.make_async_remote_copy(acc.at[t, yt], yrecv.at[t, d - 1], y_send.at[t, d - 1], y_recv.at[t, d - 1],
                                            device_id=dev(z, yt, x, c), device_id_type=MESH)

    def ystart(t):
        for d in range(1, Y):
            ycopy(t, d).start()

    def adot(t, slot):
        part = jnp.zeros((8, BOND), F32)
        for q in range(PAIR):
            prod = acc[t, q // QY, q % QY] * v[slot, q, x, 16 * t:16 * t + 16]
            part = part + prod[:8] + prod[8:]
        return part

    def acopy(stage, par, d):
        if stage == 0:
            ref, to = ay.at[y], dev(z, up(y, d, Y), x, c)
        elif stage == 1:
            ref, to = az.at[z], dev(up(z, d, Z), y, x, c)
        else:
            other_ = lax.rem(mem + d, MEMB)
            ref, to = am.at[par, mem], dev(z, y, other_ // C, lax.rem(other_, C))
        i = (0, Y - 1, Y + Z - 2)[stage] + d - 1
        return pltpu.make_async_remote_copy(ref, ref, a_send.at[par, i], a_recv.at[par, i], device_id=to, device_id_type=MESH)

    ASIZE = (Y, Z, MEMB)

    def astart(stage, par, tile):
        if stage == 0:
            ay[y] = tile
        elif stage == 1:
            az[z] = tile
        else:
            am[par, mem] = tile
        for d in range(1, ASIZE[stage]):
            acopy(stage, par, d).start()

    def adone(stage, par):
        for d in range(1, ASIZE[stage]):
            acopy(stage, par, d).wait_recv()
        tile = None
        for i in range(ASIZE[stage]):
            one_ = ay[i] if stage == 0 else az[i] if stage == 1 else am[par, i]
            tile = one_ if tile is None else tile + one_
        return tile

    def abegin(par, slot):
        part = adot(0, slot) + adot(1, slot)
        astart(0, par, part[:, :128] + part[:, 128:])

    def block(t):
        acc[t] = jnp.zeros((Y, QY, 16, BOND), F32)

        def some(kk, _):
            rest([kk * UNROLL + i for i in range(UNROLL)], [t])
            return 0
        lax.fori_loop(0, GROUP // UNROLL, some, 0)
        ystart(t)

    def tail(j, beta_prev, last):
        st = Span()
        par = lax.rem(j, 2)
        sent = []
        hz = lax.rem(z, 2)
        qz = QY * y + z // 2

        def ydone(t):
            for d in range(1, Y):
                ycopy(t, d).wait_recv()
            ysum = acc[t, y] + yrecv[t, 0] + yrecv[t, 1] + yrecv[t, 2]
            zsend[t] = ysum.reshape(Z, 8, BOND)
            zc = []
            for d in range(1, Z):
                zt = up(z, d, Z)
                zc.append(send(zsend.at[t, zt], zrecv.at[t, d - 1], z_send.at[t, d - 1], z_recv.at[t, d - 1], dev(zt, y, x, c)))
            sent.extend(zc)
            return zc

        def zdone(t, zc):
            for copy in zc:
                copy.wait_recv()
            zsum = zsend[t, z]
            for d in range(Z - 1):
                zsum = zsum + zrecv[t, d]
            s[par, qz, x, t, hz] = zsum
            ch = s.at[par, qz, x, t, hz]
            gz = [send(ch, ch, gz_send.at[par, t, d - 1], gz_recv.at[par, t, d - 1], dev(up(z, d, Z), y, x, c))
                  for d in range(1, Z)]
            sent.extend(gz)
            return gz

        slot = [0]

        def piece(part, i, k, q):
            t, h = part
            xx, yy = (k, i) if h == 0 else (i, k)
            return s.at[par, pl.ds(QY * yy + q[0], q[1]), xx, t, :, :, pl.ds(128 * h, 128)]

        qa, q0, q1 = (0, QY), (0, QY // 2), (QY // 2, QY // 2)

        def go(ref, to):
            i = slot[0]
            slot[0] += 1
            copy = send(ref, ref, gr_send.at[par, i], gr_recv.at[par, i], to)
            sent.append(copy)
            return copy

        ax = [((y, yp, ym, y2, typ, tym), (x, xp, xm, x2, txp, txm)),
              ((x, xp, xm, x2, txp, txm), (y, yp, ym, y2, typ, tym))]
        far = [dev(z, y2, x, c), dev(z, y, x2, c)]
        one, two, rel2 = {}, {}, {}

        def second(part, i, tag):
            (_, (w, _, _, _, tp, tm)) = ax[part[1]]
            two[part, tag] = [go(piece(part, i, w, qa), tp), go(piece(part, i, w, qa), tm), i]
            if tag in DIRECT2:
                two[part, tag].append(go(piece(part, i, w, qa), far[1 - part[1]]))

        def relay2(part, tag):
            (_, (w, wp, wm, _, tp, tm)) = ax[part[1]]
            cp, cm, i, *direct = two[part, tag]
            cp.wait_recv()
            if direct:
                cm.wait_recv()
                rel2[part, tag] = direct
                return
            a = go(piece(part, i, wm, q0), tp)
            cm.wait_recv()
            b = go(piece(part, i, wp, q1), tm)
            rel2[part, tag] = [a, b]

        def open_(t, gz):
            for copy in gz:
                copy.wait_recv()
            for h in (0, 1):
                ((w, _, _, _, tp, tm), (k, *_)) = ax[h]
                one[t, h] = [go(piece((t, h), w, k, qa), to) for to in (tp, tm, far[h])]
            for h in (0, 1):
                second((t, h), ax[h][0][0], "own")

        def near(t):
            for h in (0, 1):
                ((w, wp, wm, _, tp, tm), (k, *_)) = ax[h]
                one[t, h][0].wait_recv()
                second((t, h), wm, "m")
                one[t, h][1].wait_recv()
                second((t, h), wp, "p")

        def distant(t):
            for h in (0, 1):
                one[t, h][2].wait_recv()
                second((t, h), ax[h][0][3], "2")

        def relays(t, tag):
            for h in (0, 1):
                relay2((t, h), tag)

        st("rs0")
        z0 = ydone(0)
        st("rs1")
        z1 = ydone(1)
        astart(1, par, adone(0, par))
        st("z0")
        g0 = zdone(0, z0)
        st("z1")
        plane = adone(1, par)
        g1 = zdone(1, z1)
        astart(2, par, plane)
        st("g0")
        open_(0, g0)
        st("g1")
        open_(1, g1)
        st("n0")
        near(0)
        st("n1")
        near(1)
        st("o0")
        relays(0, "own")
        distant(0)
        st("o1")
        relays(1, "own")
        distant(1)
        st("ag3")
        for tag in ("m", "p", "2"):
            for t in (0, 1):
                relays(t, tag)
        for t in (0, 1):
            for tag in ("own", "m", "p", "2"):
                for h in (0, 1):
                    for copy in rel2[(t, h), tag]:
                        copy.wait_recv()
        st("sendw")
        for copy in sent:
            copy.wait_send()
        for t in (0, 1):
            for d in range(1, Y):
                ycopy(t, d).wait_send()

        st("v1")
        cur, prev = lax.rem(j, 2), lax.rem(j + 1, 2)
        tile = adone(2, par)
        alpha = jnp.sum(jnp.sum(tile, axis=0, keepdims=True), axis=1, keepdims=True) / COUNT
        for stage in range(3):
            for d in range(1, ASIZE[stage]):
                acopy(stage, par, d).wait_send()
        st("v2")

        def resid(i, t):
            w = sload(par, i) - alpha * vload(cur, i) - beta_prev * vload(prev, i)
            vstore(prev, i, w)
            return t + fold(w * w)

        part = lax.fori_loop(0, NCH, resid, jnp.zeros((8, BOND), F32), unroll=2)
        st("xb")
        beta = jnp.sqrt(both(part, 1) / COUNT)
        st("v3")
        copies = finish(prev, 1.0 / beta, j + 1)
        scalars[0, j] = alpha[0, 0]
        scalars[1, j] = beta[0, 0]
        if last:
            settle(copies, 0)
        else:
            st("stage1")
            first(copies)
            st("block0")
            block(0)
            st("block1")
            block(1)
            abegin(lax.rem(j + 1, 2), prev)
        st("")
        return beta

    sp("first")
    first(begun)
    acc[...] = jnp.zeros_like(acc)
    msib = C * x + 1 - c
    mm, mp, m2 = C * xm + c, C * xp + c, C * x2 + c
    sm, sq_, s2 = C * xm + 1 - c, C * xp + 1 - c, C * x2 + 1 - c
    base = 3 * PART

    def terms(m, h):
        return [OWN * m + PT * h + i for i in range(PT)]

    def arrive(copies, m, h, i, on=()):
        for copy in copies:
            copy.wait_recv()
        far_ = []
        for slot_, to, kinds in on:
            far_ += qsend(rall, OWN * m + PT * h, m, h, slot_, to, kinds)
        mirror(m, h)
        return far_, rsend(rpart(m, h), rpart(m, h), i, 0, sib)

    sp("R0")
    far0, a0 = arrive(from_xm[0], mm, 0, base + 3, [(base + 0, txp, (0, 1))])
    far2, b2 = arrive(from_xp[2], mp, 2, base + 8, [(base + 2, txm, (0, 1))])
    for h in range(PART):
        from_sib[h].wait_recv()
    rest([k for h in range(PART) for m in (mem, msib) for k in terms(m, h)], (0, 1))
    sp("R1")
    far1b, a1 = arrive(from_xm[1], mm, 1, base + 4, [(base + 1, txp, (1,))])
    far1a, b1 = arrive(from_xp[1], mp, 1, base + 7, [(base + 1, txm, (0,))])
    a0.wait_recv()
    b2.wait_recv()
    rest(terms(mm, 0) + terms(sm, 0) + terms(mp, 2) + terms(sq_, 2), (0, 1))
    sp("R2")
    _, a2 = arrive(from_xm[2], mm, 2, base + 5)
    _, b0 = arrive(from_xp[0], mp, 0, base + 6)
    a1.wait_recv()
    b1.wait_recv()
    rest(terms(mm, 1) + terms(sm, 1) + terms(mp, 1) + terms(sq_, 1), (0, 1))
    sp("R3")
    _, f0 = arrive(far0, m2, 0, base + 9)
    _, f2 = arrive(far2, m2, 2, base + 11)
    a2.wait_recv()
    b0.wait_recv()
    rest(terms(mm, 2) + terms(sm, 2) + terms(mp, 0) + terms(sq_, 0), (0, 1))
    sp("R4")
    _, f1 = arrive(far1a + far1b, m2, 1, base + 10)
    f0.wait_recv()
    f2.wait_recv()
    rest(terms(m2, 0) + terms(s2, 0) + terms(m2, 2) + terms(s2, 2), (0, 1))
    sp("R5")
    f1.wait_recv()
    rest(terms(m2, 1) + terms(s2, 1), (0, 1))
    for copy in early + pend:
        copy.wait_send()
    sp("")

    ystart(0)
    ystart(1)
    abegin(0, 0)

    def step(j, beta_prev):
        return tail(j, beta_prev, False)

    tail(STEPS - 1, lax.fori_loop(0, STEPS - 1, step, jnp.zeros((1, 1), F32)), True)
    mine = lax.rem(me // SLAB, C) == c
    out[...] = jnp.where(mine, rown[...], rrecv[...])


def solution(mesh):
    def local_run(psi_init, left_env, op_pair, right_env):
        dma = pltpu.SemaphoreType.DMA
        any_ = pl.BlockSpec(memory_space=pl.ANY)
        rows = pltpu.VMEM((STEPS + 1, PAIR, BOND), F32)
        out, scalars = pl.pallas_call(
            kernel,
            out_shape=(jax.ShapeDtypeStruct((STEPS + 1, PAIR, BOND), F32),
                       jax.ShapeDtypeStruct((2, STEPS), F32)),
            in_specs=[any_] * 4,
            out_specs=(pl.BlockSpec(memory_space=pltpu.VMEM),
                       pl.BlockSpec(memory_space=pltpu.SMEM)),
            scratch_shapes=[
                pltpu.VMEM((GROUP, SLAB, BOND), BF16),
                pltpu.VMEM((GROUP, PAIR, PAIR), BF16),
                pltpu.VMEM((GROUP, PAIR, 256), F32),
                pltpu.VMEM((GROUP, BOND, BOND), BF16),
                pltpu.VMEM((GROUP, 256, 256), BF16),
                pltpu.VMEM((PAIR, GROUP, SLAB, BOND), BF16),
                pltpu.VMEM((PAIR, X, C, SLAB, BOND), BF16),
                pltpu.VMEM((2, PAIR, X, SLAB, BOND), F32),
                pltpu.VMEM((2, PAIR, X, 2, 2, 8, BOND), F32),
                pltpu.VMEM((2, Y, QY, 16, BOND), F32),
                pltpu.VMEM((2, Y - 1, QY, 16, BOND), F32),
                pltpu.VMEM((2, Z, 8, BOND), F32),
                pltpu.VMEM((2, Z - 1, 8, BOND), F32),
                pltpu.VMEM((2, 8, 128), F32),
                pltpu.VMEM((2, 8, 128), F32),
                pltpu.VMEM((Y, 8, 128), F32),
                pltpu.VMEM((Z, 8, 128), F32),
                pltpu.VMEM((2, MEMB, 8, 128), F32),
                rows, rows, rows,
                dma((20,)), dma((2, 7)), dma((2, 7)),
                dma((21, 2)), dma((21, 2)),
                dma((2, 3)), dma((2, 3)), dma((2, 7)), dma((2, 7)),
                dma((2, 2, 7)), dma((2, 2, 7)),
                dma((2, 80)), dma((2, 80)),
                dma((2,)), dma((2,)),
                dma((2, 17)), dma((2, 17)),
                dma((4,)), dma((4,)),
                dma((1,)), dma((1,)),
            ],
            compiler_params=pltpu.CompilerParams(
                collective_id=0, has_side_effects=True, vmem_limit_bytes=66 * 1000 * 1000),
        )(psi_init.reshape(X, C, SLAB, 4, 4, BOND), left_env, op_pair, right_env)
        return out.reshape(STEPS + 1, 1, 4, 4, BOND), scalars[0], scalars[1]

    return jax.shard_map(local_run, mesh=mesh, in_specs=(P(), P("terms"), P("terms"), P("terms")),
                         out_specs=(P(None, "terms"), P(), P()), check_vma=False)
```

```python
import jax
import jax.numpy as jnp
from jax import lax
from jax.experimental import pallas as pl
from jax.experimental.pallas import tpu as pltpu
from jax.sharding import PartitionSpec as P

STEPS = 6
Z, Y, X, C = 8, 4, 4, 2
BOND, PAIR = 256, 16
OWN = 6
MEMB = X * C
GROUP = OWN * MEMB
SLAB = BOND // MEMB
PART = 3
PT = OWN // PART
COUNT = BOND * PAIR * BOND
UNROLL = 24
QY = PAIR // Y
DIRECT2 = ((), ("2",))
F32, BF16 = jnp.float32, jnp.bfloat16
MESH = pl.DeviceIdType.MESH


class Span:
    def __init__(self):
        self.open = None

    def __call__(self, name):
        if self.open is not None:
            self.open.__exit__(None, None, None)
        self.open = None
        if name:
            self.open = jax.named_scope(name)
            self.open.__enter__()


def kernel(psi, left, ops, right, out, scalars,
           lst, wall, wide, rall, kron, u, vb, v, s, acc, accin, yrecv, zsend, zrecv, ssend, srecv, ay, az, am, rown, rsib, rrecv,
           loc_sem, l_send, l_recv, r_send, r_recv, x_send, x_recv, y_send, y_recv, z_send, z_recv,
           gz_send, gz_recv, gr_send, gr_recv, c_send, c_recv, a_send, a_recv, b_send, b_recv, row_send, row_recv):
    me = lax.axis_index("terms")
    sp = Span()
    c = lax.rem(me, C)
    x = lax.rem(me // C, X)
    y = lax.rem(me // (C * X), Y)
    z = me // (C * X * Y)
    mem = lax.rem(me, MEMB)

    def dev(zz, yy, xx, cc):
        return (((zz * Y + yy) * X + xx) * C + cc,)

    def up(pos, step, size):
        return lax.rem(pos + step, size)

    def send(src, dst, ssem, rsem, to):
        copy = pltpu.make_async_remote_copy(src, dst, ssem, rsem, device_id=to, device_id_type=MESH)
        copy.start()
        return copy

    xp, xm, x2 = up(x, 1, X), up(x, X - 1, X), up(x, 2, X)
    yp, ym, y2 = up(y, 1, Y), up(y, Y - 1, Y), up(y, 2, Y)
    sib = dev(z, y, x, 1 - c)
    txp, txm = dev(z, y, xp, c), dev(z, y, xm, c)
    typ, tym = dev(z, yp, x, c), dev(z, ym, x, c)

    sp("entry")
    barrier = pltpu.get_barrier_semaphore()
    peers = [dev(up(z, d, Z), y, x, c) for d in range(1, Z)]
    peers += [dev(z, up(y, d, Y), x, c) for d in range(1, Y)]
    peers += [dev(z, y, up(x, d, X), cc) for d in range(1, X) for cc in range(C)]
    peers += [sib]
    for peer in peers:
        pl.semaphore_signal(barrier, inc=1, device_id=peer, device_id_type=MESH)
    own = pl.ds(OWN * mem, OWN)
    local = [pltpu.make_async_copy(psi.at[:, :, c, :, p // 4, p % 4, :], v.at[0, p], loc_sem.at[4 + p]) for p in range(PAIR)]
    local = local[::-1] + [
             pltpu.make_async_copy(left.at[:, pl.ds(pl.multiple_of(SLAB * mem, SLAB), SLAB)], lst.at[own], loc_sem.at[1]),
             pltpu.make_async_copy(right, rall.at[own], loc_sem.at[2]),
             pltpu.make_async_copy(ops, wall.at[own], loc_sem.at[3])]
    for copy in local:
        copy.start()
    pl.semaphore_wait(barrier, len(peers))

    early = []
    for d in range(MEMB - 1):
        to = lax.rem(mem + 1 + d, MEMB)
        early.append(send(left.at[:, pl.ds(pl.multiple_of(SLAB * to, SLAB), SLAB)], lst.at[own],
                          l_send.at[0, d], l_recv.at[0, d], dev(z, y, to // C, lax.rem(to, C))))
        early.append(send(ops, wall.at[own], l_send.at[1, d], l_recv.at[1, d],
                          dev(z, y, to // C, lax.rem(to, C))))

    def rpart(m, h):
        return rall.at[pl.ds(OWN * m + PT * h, PT)]

    pend = []
    H = BOND // 2

    def quads(ref, k0):
        return ref.at[pl.ds(k0, PT), pl.ds(0, H)], ref.at[pl.ds(k0, PT), pl.ds(H, H), pl.ds(H, H)]

    def rsend(src, dst, i, kind, to):
        copy = send(src, dst, r_send.at[i, kind], r_recv.at[i, kind], to)
        pend.append(copy)
        return copy

    def qsend(src, k0, m, h, i, to, kinds=(0, 1)):
        a, b = quads(src, k0), quads(rall, OWN * m + PT * h)
        return [rsend(a[kind], b[kind], i, kind, to) for kind in kinds]

    def mirror(m, h):
        for i in range(PT):
            k = OWN * m + PT * h + i
            rall[k, H:, :H] = rall[k, :H, H:].T

    def rpart(m, h):
        return rall.at[pl.ds(OWN * m + PT * h, PT)]

    from_xm, from_xp, from_sib = {}, {}, {}
    for h in range(PART):
        g = PART - 1 - h
        from_xm[h] = qsend(right, PT * h, mem, h, h, txp)
        from_xp[g] = qsend(right, PT * g, mem, g, PART + g, txm)
    for h in range(PART):
        from_sib[h] = rsend(right.at[pl.ds(PT * h, PT)], rpart(mem, h), 2 * PART + h, 0, sib)

    def chunk(i):
        return i // 2, pl.ds((i % 2) * 2, 2)

    NCH = 2 * PAIR

    def vload(slot, i):
        q, xx = chunk(i)
        return v[slot, q, xx].reshape(64, BOND)

    def vstore(slot, i, val):
        q, xx = chunk(i)
        v[slot, q, xx] = val.reshape(2, C, 16, BOND)

    def sload(par, i):
        q, xx = chunk(i)
        return s[par, q, xx].reshape(64, BOND)

    def fold(t):
        return jnp.sum(t.reshape(8, 8, BOND), axis=0)

    def both(part, i):
        tile = part[:, :128] + part[:, 128:]
        ssend[i] = tile
        copy = send(ssend.at[i], srecv.at[i], c_send.at[i], c_recv.at[i], sib)
        copy.wait()
        t = tile + srecv[i]
        return jnp.sum(jnp.sum(t, axis=0, keepdims=True), axis=1, keepdims=True)

    inhalf = me // (BOND // X)

    other = me + 1 - 2 * c
    QG = PAIR // 4

    def vbcopy(g):
        ref = vb.at[pl.ds(QG * g, QG), :, :, c]
        return pltpu.make_async_remote_copy(ref, ref, b_send.at[g], b_recv.at[g], device_id=sib, device_id_type=MESH)

    def finish(slot, inv, row):
        copies = []
        for g in range(4):
            def one(i, _):
                w = vload(slot, i) * inv
                vstore(slot, i, w)
                q, xx = chunk(i)
                vb[q, xx, :, c] = w.astype(BF16).reshape(2, C, 16, BOND)
                return 0
            lax.fori_loop(NCH // 4 * g, NCH // 4 * (g + 1), one, 0, unroll=2)
            copies.append(vbcopy(g))
            copies[-1].start()

        def pick(q, _):
            rown[row, pl.ds(q, 1)] = v[slot, q, inhalf, lax.rem(me // SLAB, C), pl.ds(lax.rem(me, 16), 1)]
            rsib[row, pl.ds(q, 1)] = v[slot, q, inhalf, lax.rem(me // SLAB, C), pl.ds(lax.rem(other, 16), 1)]
            return 0

        lax.fori_loop(0, PAIR, pick, 0, unroll=4)
        copies.append(send(rsib.at[row], rrecv.at[row], row_send.at[0], row_recv.at[0], sib))
        return copies

    def first(copies):
        rows = lst[...].reshape(GROUP * SLAB, BOND)
        for g in range(4):
            copies[g].wait_recv()
            for p in range(QG * g, QG * g + QG):
                w = jnp.dot(rows, vb[p].reshape(BOND, BOND), preferred_element_type=F32)
                u[p] = w.astype(BF16).reshape(GROUP, SLAB, BOND)
        settle(copies, 4)

    def settle(copies, n):
        for copy in copies[n:]:
            copy.wait_recv()
        for copy in copies:
            copy.wait_send()

    sp("init")
    for copy in local:
        copy.wait()

    def sq(i, t):
        blk = vload(0, i)
        return t + fold(blk * blk)

    def clear(i, _):
        vstore(1, i, jnp.zeros((64, BOND), F32))
        return 0

    lax.fori_loop(0, NCH, clear, 0)
    part = lax.fori_loop(0, NCH, sq, jnp.zeros((8, BOND), F32), unroll=2)
    nrm = jnp.sqrt(both(part, 0) / COUNT)
    begun = finish(0, 1.0 / nrm, 0)

    sp("waitL")
    for copy in early:
        copy.wait_recv()
    sp("build")
    lane = lax.broadcasted_iota(jnp.int32, (16, 256), 1) % 16
    rowi = lax.broadcasted_iota(jnp.int32, (16, 256), 0)
    diag = lane == rowi

    spread = lax.broadcasted_iota(jnp.int32, (PAIR, 256), 0) == lax.broadcasted_iota(jnp.int32, (PAIR, 256), 1) // 16
    rows = jnp.dot(wall[...].reshape(GROUP * PAIR, PAIR), spread.astype(F32).astype(BF16), preferred_element_type=F32)
    wide[...] = rows.reshape(GROUP, PAIR, 256)

    def build(k, _):
        wk = wide[k]
        for q in range(PAIR):
            blk = jnp.where(diag, jnp.broadcast_to(wk[q:q + 1], (16, 256)), 0.0)
            kron[k, 16 * q:16 * q + 16] = blk.astype(BF16)
        return 0

    lax.fori_loop(0, GROUP, build, 0)

    def rest(ks, ts):
        res = None
        for k in ks:
            zs = []
            for t in ts:
                blk = u[:, k, 16 * t:16 * t + 16].reshape(256, BOND)
                zs.append(jnp.dot(kron[k], blk, preferred_element_type=F32).astype(BF16))
            zk = zs[0] if len(zs) == 1 else jnp.concatenate(zs, axis=0)
            o = jnp.dot(zk, rall[k], preferred_element_type=F32)
            res = o if res is None else res + o
        for i, t in enumerate(ts):
            acc[t] += res[256 * i:256 * i + 256].reshape(Y, QY, 16, BOND)

    slab = (c, 1 - c)

    def handover():
        return pltpu.make_async_remote_copy(acc.at[1 - c], accin, x_send.at[0], x_recv.at[0],
                                            device_id=sib, device_id_type=MESH)

    def mine_(t, *i):
        return acc[(c, *i)] if t == 0 else accin[i]

    def ycopy(t, d):
        yt = up(y, d, Y)
        return pltpu.make_async_remote_copy(acc.at[c, yt] if t == 0 else accin.at[yt], yrecv.at[t, d - 1], y_send.at[t, d - 1], y_recv.at[t, d - 1],
                                            device_id=dev(z, yt, x, c), device_id_type=MESH)

    def ystart(t):
        for d in range(1, Y):
            ycopy(t, d).start()

    def adot(t, slot):
        part = jnp.zeros((8, BOND), F32)
        for q in range(PAIR):
            prod = mine_(t, q // QY, q % QY) * v[slot, q, x, slab[t]]
            part = part + prod[:8] + prod[8:]
        return part

    def acopy(stage, par, d):
        if stage == 0:
            ref, to = ay.at[par, y], dev(z, up(y, d, Y), x, c)
        elif stage == 1:
            ref, to = az.at[par, z], dev(up(z, d, Z), y, x, c)
        else:
            other_ = lax.rem(mem + d, MEMB)
            ref, to = am.at[par, mem], dev(z, y, other_ // C, lax.rem(other_, C))
        i = (0, Y - 1, Y + Z - 2)[stage] + d - 1
        return pltpu.make_async_remote_copy(ref, ref, a_send.at[par, i], a_recv.at[par, i], device_id=to, device_id_type=MESH)

    ASIZE = (Y, Z, MEMB)

    def astart(stage, par, tile):
        if stage == 0:
            ay[par, y] = tile
        elif stage == 1:
            az[par, z] = tile
        else:
            am[par, mem] = tile
        for d in range(1, ASIZE[stage]):
            acopy(stage, par, d).start()

    def adone(stage, par):
        for d in range(1, ASIZE[stage]):
            acopy(stage, par, d).wait_recv()
        tile = None
        for i in range(ASIZE[stage]):
            one_ = ay[par, i] if stage == 0 else az[par, i] if stage == 1 else am[par, i]
            tile = one_ if tile is None else tile + one_
        return tile

    def abegin(par, slot):
        part = adot(0, slot) + adot(1, slot)
        astart(0, par, part[:, :128] + part[:, 128:])

    def on(core, *acts):
        @pl.when(c == core)
        def _():
            for act in acts:
                act()

    def take():
        handover().wait_recv()
        ystart(1)

    def blocks():
        acc[...] = jnp.zeros_like(acc)

        rest(list(range(GROUP)), [0])
        on(1, lambda: handover().start())
        on(0, lambda: ystart(0))
        rest(list(range(UNROLL)), [1])
        on(0, take)
        rest(list(range(UNROLL, GROUP)), [1])
        on(1, lambda: ystart(0))
        on(0, lambda: handover().start())

    def tail(j, beta_prev, last):
        st = Span()
        par = lax.rem(j, 2)
        sent = []
        hz = lax.rem(z, 2)
        qz = QY * y + z // 2

        def ydone(t):
            for d in range(1, Y):
                ycopy(t, d).wait_recv()
            ysum = mine_(t, y) + yrecv[t, 0] + yrecv[t, 1] + yrecv[t, 2]
            zsend[t] = ysum.reshape(Z, 8, BOND)
            zc = []
            for d in range(1, Z):
                zt = up(z, d, Z)
                zc.append(send(zsend.at[t, zt], zrecv.at[t, d - 1], z_send.at[t, d - 1], z_recv.at[t, d - 1], dev(zt, y, x, c)))
            sent.extend(zc)
            return zc

        def zdone(t, zc):
            for copy in zc:
                copy.wait_recv()
            zsum = zsend[t, z]
            for d in range(Z - 1):
                zsum = zsum + zrecv[t, d]
            s[par, qz, x, slab[t], hz] = zsum
            ch = s.at[par, qz, x, slab[t], hz]
            gz = [send(ch, ch, gz_send.at[par, t, d - 1], gz_recv.at[par, t, d - 1], dev(up(z, d, Z), y, x, c))
                  for d in range(1, Z)]
            sent.extend(gz)
            return gz

        slot = [0]

        def piece(part, i, k, q):
            t, h = part
            xx, yy = (k, i) if h == 0 else (i, k)
            return s.at[par, pl.ds(QY * yy + q[0], q[1]), xx, slab[t], :, :, pl.ds(128 * h, 128)]

        qa, q0, q1 = (0, QY), (0, QY // 2), (QY // 2, QY // 2)

        def go(ref, to):
            i = slot[0]
            slot[0] += 1
            copy = send(ref, ref, gr_send.at[par, i], gr_recv.at[par, i], to)
            sent.append(copy)
            return copy

        ax = [((y, yp, ym, y2, typ, tym), (x, xp, xm, x2, txp, txm)),
              ((x, xp, xm, x2, txp, txm), (y, yp, ym, y2, typ, tym))]
        far = [dev(z, y2, x, c), dev(z, y, x2, c)]
        one, two, rel2 = {}, {}, {}

        def second(part, i, tag):
            (_, (w, _, _, _, tp, tm)) = ax[part[1]]
            two[part, tag] = [go(piece(part, i, w, qa), tp), go(piece(part, i, w, qa), tm), i]
            if tag in DIRECT2[part[0]]:
                two[part, tag].append(go(piece(part, i, w, qa), far[1 - part[1]]))

        def relay2(part, tag):
            (_, (w, wp, wm, _, tp, tm)) = ax[part[1]]
            cp, cm, i, *direct = two[part, tag]
            cp.wait_recv()
            if direct:
                cm.wait_recv()
                rel2[part, tag] = direct
                return
            a = go(piece(part, i, wm, q0), tp)
            cm.wait_recv()
            b = go(piece(part, i, wp, q1), tm)
            rel2[part, tag] = [a, b]

        def open_(t, gz):
            for copy in gz:
                copy.wait_recv()
            for h in (0, 1):
                ((w, _, _, _, tp, tm), (k, *_)) = ax[h]
                one[t, h] = [go(piece((t, h), w, k, qa), to) for to in (tp, tm, far[h])]
            for h in (0, 1):
                second((t, h), ax[h][0][0], "own")

        def near(t):
            for h in (0, 1):
                ((w, wp, wm, _, tp, tm), (k, *_)) = ax[h]
                one[t, h][0].wait_recv()
                second((t, h), wm, "m")
                one[t, h][1].wait_recv()
                second((t, h), wp, "p")

        def distant(t):
            for h in (0, 1):
                one[t, h][2].wait_recv()
                second((t, h), ax[h][0][3], "2")

        def relays(t, tag):
            for h in (0, 1):
                relay2((t, h), tag)

        st("take")
        on(1, take)
        abegin(par, par)
        st("rs0")
        z0 = ydone(0)
        st("rs1")
        z1 = ydone(1)
        st("z0")
        g0 = zdone(0, z0)
        astart(1, par, adone(0, par))
        st("z1")
        g1 = zdone(1, z1)
        st("g0")
        open_(0, g0)
        st("g1")
        open_(1, g1)
        astart(2, par, adone(1, par))
        st("n0")
        near(0)
        st("n1")
        near(1)
        st("o0")
        relays(0, "own")
        distant(0)
        st("o1")
        relays(1, "own")
        distant(1)
        st("ag3")
        for tag in ("m", "p", "2"):
            for t in (0, 1):
                relays(t, tag)
        for t in (0, 1):
            for tag in ("own", "m", "p", "2"):
                for h in (0, 1):
                    for copy in rel2[(t, h), tag]:
                        copy.wait_recv()
        st("sendw")
        for copy in sent:
            copy.wait_send()
        for t in (0, 1):
            for d in range(1, Y):
                ycopy(t, d).wait_send()
        handover().wait_send()

        st("v1")
        cur, prev = lax.rem(j, 2), lax.rem(j + 1, 2)
        tile = adone(2, par)
        alpha = jnp.sum(jnp.sum(tile, axis=0, keepdims=True), axis=1, keepdims=True) / COUNT
        for stage in range(3):
            for d in range(1, ASIZE[stage]):
                acopy(stage, par, d).wait_send()
        st("v2")

        def resid(i, t):
            w = sload(par, i) - alpha * vload(cur, i) - beta_prev * vload(prev, i)
            vstore(prev, i, w)
            return t + fold(w * w)

        part = lax.fori_loop(0, NCH, resid, jnp.zeros((8, BOND), F32), unroll=2)
        st("xb")
        beta = jnp.sqrt(both(part, 1) / COUNT)
        st("v3")
        copies = finish(prev, 1.0 / beta, j + 1)
        scalars[0, j] = alpha[0, 0]
        scalars[1, j] = beta[0, 0]
        if last:
            settle(copies, 0)
        else:
            st("stage1")
            first(copies)
            st("blocks")
            blocks()
        st("")
        return beta

    sp("first")
    first(begun)
    acc[...] = jnp.zeros_like(acc)
    msib = C * x + 1 - c
    mm, mp, m2 = C * xm + c, C * xp + c, C * x2 + c
    sm, sq_, s2 = C * xm + 1 - c, C * xp + 1 - c, C * x2 + 1 - c
    base = 3 * PART

    def terms(m, h):
        return [OWN * m + PT * h + i for i in range(PT)]

    def arrive(copies, m, h, i, on=()):
        for copy in copies:
            copy.wait_recv()
        far_ = []
        for slot_, to, kinds in on:
            far_ += qsend(rall, OWN * m + PT * h, m, h, slot_, to, kinds)
        mirror(m, h)
        return far_, rsend(rpart(m, h), rpart(m, h), i, 0, sib)

    sp("R0")
    far0, a0 = arrive(from_xm[0], mm, 0, base + 3, [(base + 0, txp, (0, 1))])
    far2, b2 = arrive(from_xp[2], mp, 2, base + 8, [(base + 2, txm, (0, 1))])
    for h in range(PART):
        from_sib[h].wait_recv()
    rest([k for h in range(PART) for m in (mem, msib) for k in terms(m, h)], (0, 1))
    sp("R1")
    far1b, a1 = arrive(from_xm[1], mm, 1, base + 4, [(base + 1, txp, (1,))])
    far1a, b1 = arrive(from_xp[1], mp, 1, base + 7, [(base + 1, txm, (0,))])
    a0.wait_recv()
    b2.wait_recv()
    rest(terms(mm, 0) + terms(sm, 0) + terms(mp, 2) + terms(sq_, 2), (0, 1))
    sp("R2")
    _, a2 = arrive(from_xm[2], mm, 2, base + 5)
    _, b0 = arrive(from_xp[0], mp, 0, base + 6)
    a1.wait_recv()
    b1.wait_recv()
    rest(terms(mm, 1) + terms(sm, 1) + terms(mp, 1) + terms(sq_, 1), (0, 1))
    sp("R3")
    _, f0 = arrive(far0, m2, 0, base + 9)
    _, f2 = arrive(far2, m2, 2, base + 11)
    a2.wait_recv()
    b0.wait_recv()
    rest(terms(mm, 2) + terms(sm, 2) + terms(mp, 0) + terms(sq_, 0), (0, 1))
    sp("R4")
    _, f1 = arrive(far1a + far1b, m2, 1, base + 10)
    f0.wait_recv()
    f2.wait_recv()
    rest(terms(m2, 0) + terms(s2, 0) + terms(m2, 2) + terms(s2, 2), (0, 1))
    sp("R5")
    f1.wait_recv()
    rest(terms(m2, 1) + terms(s2, 1), (0, 1))
    for copy in early + pend:
        copy.wait_send()
    sp("")

    handover().start()
    ystart(0)
    on(0, take)

    def step(j, beta_prev):
        return tail(j, beta_prev, False)

    tail(STEPS - 1, lax.fori_loop(0, STEPS - 1, step, jnp.zeros((1, 1), F32)), True)
    mine = lax.rem(me // 16, 2) == c
    out[...] = jnp.where(mine, rown[...], rrecv[...])


def solution(mesh):
    def local_run(psi_init, left_env, op_pair, right_env):
        dma = pltpu.SemaphoreType.DMA
        any_ = pl.BlockSpec(memory_space=pl.ANY)
        rows = pltpu.VMEM((STEPS + 1, PAIR, BOND), F32)
        out, scalars = pl.pallas_call(
            kernel,
            out_shape=(jax.ShapeDtypeStruct((STEPS + 1, PAIR, BOND), F32),
                       jax.ShapeDtypeStruct((2, STEPS), F32)),
            in_specs=[any_] * 4,
            out_specs=(pl.BlockSpec(memory_space=pltpu.VMEM),
                       pl.BlockSpec(memory_space=pltpu.SMEM)),
            scratch_shapes=[
                pltpu.VMEM((GROUP, SLAB, BOND), BF16),
                pltpu.VMEM((GROUP, PAIR, PAIR), BF16),
                pltpu.VMEM((GROUP, PAIR, 256), F32),
                pltpu.VMEM((GROUP, BOND, BOND), BF16),
                pltpu.VMEM((GROUP, 256, 256), BF16),
                pltpu.VMEM((PAIR, GROUP, SLAB, BOND), BF16),
                pltpu.VMEM((PAIR, X, C, 2, 16, BOND), BF16),
                pltpu.VMEM((2, PAIR, X, C, 16, BOND), F32),
                pltpu.VMEM((2, PAIR, X, C, 2, 8, BOND), F32),
                pltpu.VMEM((2, Y, QY, 16, BOND), F32),
                pltpu.VMEM((Y, QY, 16, BOND), F32),
                pltpu.VMEM((2, Y - 1, QY, 16, BOND), F32),
                pltpu.VMEM((2, Z, 8, BOND), F32),
                pltpu.VMEM((2, Z - 1, 8, BOND), F32),
                pltpu.VMEM((2, 8, 128), F32),
                pltpu.VMEM((2, 8, 128), F32),
                pltpu.VMEM((2, Y, 8, 128), F32),
                pltpu.VMEM((2, Z, 8, 128), F32),
                pltpu.VMEM((2, MEMB, 8, 128), F32),
                rows, rows, rows,
                dma((20,)), dma((2, 7)), dma((2, 7)),
                dma((21, 2)), dma((21, 2)),
                dma((1,)), dma((1,)),
                dma((2, 3)), dma((2, 3)), dma((2, 7)), dma((2, 7)),
                dma((2, 2, 7)), dma((2, 2, 7)),
                dma((2, 80)), dma((2, 80)),
                dma((2,)), dma((2,)),
                dma((2, 17)), dma((2, 17)),
                dma((4,)), dma((4,)),
                dma((1,)), dma((1,)),
            ],
            compiler_params=pltpu.CompilerParams(
                collective_id=0, has_side_effects=True, vmem_limit_bytes=66 * 1000 * 1000),
        )(psi_init.reshape(X, C, 2, 16, 4, 4, BOND), left_env, op_pair, right_env)
        return out.reshape(STEPS + 1, 1, 4, 4, BOND), scalars[0], scalars[1]

    return jax.shard_map(local_run, mesh=mesh, in_specs=(P(), P("terms"), P("terms"), P("terms")),
                         out_specs=(P(None, "terms"), P(), P()), check_vma=False)
```

```python
import jax
import jax.numpy as jnp
from jax import lax
from jax.experimental import pallas as pl
from jax.experimental.pallas import tpu as pltpu
from jax.sharding import PartitionSpec as P

STEPS = 6
Z, Y, X, C = 8, 4, 4, 2
BOND, PAIR = 256, 16
OWN = 6
MEMB = X * C
GROUP = OWN * MEMB
SLAB = BOND // MEMB
PART = 3
PT = OWN // PART
COUNT = BOND * PAIR * BOND
UNROLL = 24
PLANE = Y * X * C
QY = PAIR // Y
DIRECT2 = ((), ("2",))
F32, BF16 = jnp.float32, jnp.bfloat16
MESH = pl.DeviceIdType.MESH


class Span:
    def __init__(self):
        self.open = None

    def __call__(self, name):
        if self.open is not None:
            self.open.__exit__(None, None, None)
        self.open = None
        if name:
            self.open = jax.named_scope(name)
            self.open.__enter__()


def kernel(psi, left, ops, right, out, scalars,
           lst, wall, wide, rall, kron, u, vb, v, s, acc, accin, yrecv, zsend, zrecv, ssend, srecv, pm, zm, rown, rsib, rrecv,
           loc_sem, l_send, l_recv, r_send, r_recv, x_send, x_recv, y_send, y_recv, z_send, z_recv,
           gz_send, gz_recv, gr_send, gr_recv, c_send, c_recv, p_send, p_recv, a_send, a_recv, b_send, b_recv, row_send, row_recv):
    me = lax.axis_index("terms")
    sp = Span()
    c = lax.rem(me, C)
    x = lax.rem(me // C, X)
    y = lax.rem(me // (C * X), Y)
    z = me // (C * X * Y)
    mem = lax.rem(me, MEMB)

    def dev(zz, yy, xx, cc):
        return (((zz * Y + yy) * X + xx) * C + cc,)

    def up(pos, step, size):
        return lax.rem(pos + step, size)

    def send(src, dst, ssem, rsem, to):
        copy = pltpu.make_async_remote_copy(src, dst, ssem, rsem, device_id=to, device_id_type=MESH)
        copy.start()
        return copy

    xp, xm, x2 = up(x, 1, X), up(x, X - 1, X), up(x, 2, X)
    yp, ym, y2 = up(y, 1, Y), up(y, Y - 1, Y), up(y, 2, Y)
    sib = dev(z, y, x, 1 - c)
    txp, txm = dev(z, y, xp, c), dev(z, y, xm, c)
    typ, tym = dev(z, yp, x, c), dev(z, ym, x, c)

    sp("entry")
    barrier = pltpu.get_barrier_semaphore()
    peers = [dev(up(z, d, Z), y, x, c) for d in range(1, Z)]
    place = lax.rem(me, PLANE)
    peers += [(PLANE * z + lax.rem(place + d, PLANE),) for d in range(1, PLANE)]
    for peer in peers:
        pl.semaphore_signal(barrier, inc=1, device_id=peer, device_id_type=MESH)
    own = pl.ds(OWN * mem, OWN)
    local = [pltpu.make_async_copy(psi.at[:, :, c, :, p // 4, p % 4, :], v.at[0, p], loc_sem.at[4 + p]) for p in range(PAIR)]
    local = local[::-1] + [
             pltpu.make_async_copy(left.at[:, pl.ds(pl.multiple_of(SLAB * mem, SLAB), SLAB)], lst.at[own], loc_sem.at[1]),
             pltpu.make_async_copy(right, rall.at[own], loc_sem.at[2]),
             pltpu.make_async_copy(ops, wall.at[own], loc_sem.at[3])]
    for copy in local:
        copy.start()
    pl.semaphore_wait(barrier, len(peers))

    early = []
    for d in range(MEMB - 1):
        to = lax.rem(mem + 1 + d, MEMB)
        early.append(send(left.at[:, pl.ds(pl.multiple_of(SLAB * to, SLAB), SLAB)], lst.at[own],
                          l_send.at[0, d], l_recv.at[0, d], dev(z, y, to // C, lax.rem(to, C))))
        early.append(send(ops, wall.at[own], l_send.at[1, d], l_recv.at[1, d],
                          dev(z, y, to // C, lax.rem(to, C))))

    def rpart(m, h):
        return rall.at[pl.ds(OWN * m + PT * h, PT)]

    pend = []
    H = BOND // 2

    def quads(ref, k0):
        return ref.at[pl.ds(k0, PT), pl.ds(0, H)], ref.at[pl.ds(k0, PT), pl.ds(H, H), pl.ds(H, H)]

    def rsend(src, dst, i, kind, to):
        copy = send(src, dst, r_send.at[i, kind], r_recv.at[i, kind], to)
        pend.append(copy)
        return copy

    def qsend(src, k0, m, h, i, to, kinds=(0, 1)):
        a, b = quads(src, k0), quads(rall, OWN * m + PT * h)
        return [rsend(a[kind], b[kind], i, kind, to) for kind in kinds]

    def mirror(m, h):
        for i in range(PT):
            k = OWN * m + PT * h + i
            rall[k, H:, :H] = rall[k, :H, H:].T

    def rpart(m, h):
        return rall.at[pl.ds(OWN * m + PT * h, PT)]

    from_xm, from_xp, from_sib = {}, {}, {}
    for h in range(PART):
        g = PART - 1 - h
        from_xm[h] = qsend(right, PT * h, mem, h, h, txp)
        from_xp[g] = qsend(right, PT * g, mem, g, PART + g, txm)
    for h in range(PART):
        from_sib[h] = rsend(right.at[pl.ds(PT * h, PT)], rpart(mem, h), 2 * PART + h, 0, sib)

    def chunk(i):
        return i // 2, pl.ds((i % 2) * 2, 2)

    NCH = 2 * PAIR

    def vload(slot, i):
        q, xx = chunk(i)
        return v[slot, q, xx].reshape(64, BOND)

    def vstore(slot, i, val):
        q, xx = chunk(i)
        v[slot, q, xx] = val.reshape(2, C, 16, BOND)

    def sload(par, i):
        q, xx = chunk(i)
        return s[par, q, xx].reshape(64, BOND)

    def fold(t):
        return jnp.sum(t.reshape(8, 8, BOND), axis=0)

    def both(part):
        tile = part[:, :128] + part[:, 128:]
        ssend[...] = tile
        send(ssend, srecv, c_send.at[0], c_recv.at[0], sib).wait()
        t = tile + srecv[...]
        return jnp.sum(jnp.sum(t, axis=0, keepdims=True), axis=1, keepdims=True)

    inhalf = me // (BOND // X)

    other = me + 1 - 2 * c
    QG = PAIR // 4

    def vbcopy(g):
        ref = vb.at[pl.ds(QG * g, QG), :, :, c]
        return pltpu.make_async_remote_copy(ref, ref, b_send.at[g], b_recv.at[g], device_id=sib, device_id_type=MESH)

    def finish(slot, value, row):
        copies = []
        for g in range(4):
            def one(i, _):
                w = value(i)
                vstore(slot, i, w)
                q, xx = chunk(i)
                vb[q, xx, :, c] = w.astype(BF16).reshape(2, C, 16, BOND)
                return 0
            lax.fori_loop(NCH // 4 * g, NCH // 4 * (g + 1), one, 0, unroll=2)
            copies.append(vbcopy(g))
            copies[-1].start()

        def pick(q, _):
            rown[row, pl.ds(q, 1)] = v[slot, q, inhalf, lax.rem(me // SLAB, C), pl.ds(lax.rem(me, 16), 1)]
            rsib[row, pl.ds(q, 1)] = v[slot, q, inhalf, lax.rem(me // SLAB, C), pl.ds(lax.rem(other, 16), 1)]
            return 0

        lax.fori_loop(0, PAIR, pick, 0, unroll=4)
        copies.append(send(rsib.at[row], rrecv.at[row], row_send.at[0], row_recv.at[0], sib))
        return copies

    def first(copies):
        rows = lst[...].reshape(GROUP * SLAB, BOND)
        for g in range(4):
            copies[g].wait_recv()
            for p in range(QG * g, QG * g + QG):
                w = jnp.dot(rows, vb[p].reshape(BOND, BOND), preferred_element_type=F32)
                u[p] = w.astype(BF16).reshape(GROUP, SLAB, BOND)
        settle(copies, 4)

    def settle(copies, n):
        for copy in copies[n:]:
            copy.wait_recv()
        for copy in copies:
            copy.wait_send()

    sp("init")
    for copy in local:
        copy.wait()

    def sq(i, t):
        blk = vload(0, i)
        return t + fold(blk * blk)

    def clear(i, _):
        vstore(1, i, jnp.zeros((64, BOND), F32))
        return 0

    lax.fori_loop(0, NCH, clear, 0)
    part = lax.fori_loop(0, NCH, sq, jnp.zeros((8, BOND), F32), unroll=2)
    nrm = jnp.sqrt(both(part) / COUNT)
    inv0 = 1.0 / nrm
    begun = finish(0, lambda i: vload(0, i) * inv0, 0)

    sp("waitL")
    for copy in early:
        copy.wait_recv()
    sp("build")
    lane = lax.broadcasted_iota(jnp.int32, (16, 256), 1) % 16
    rowi = lax.broadcasted_iota(jnp.int32, (16, 256), 0)
    diag = lane == rowi

    spread = lax.broadcasted_iota(jnp.int32, (PAIR, 256), 0) == lax.broadcasted_iota(jnp.int32, (PAIR, 256), 1) // 16
    rows = jnp.dot(wall[...].reshape(GROUP * PAIR, PAIR), spread.astype(F32).astype(BF16), preferred_element_type=F32)
    wide[...] = rows.reshape(GROUP, PAIR, 256)

    def build(k, _):
        wk = wide[k]
        for q in range(PAIR):
            blk = jnp.where(diag, jnp.broadcast_to(wk[q:q + 1], (16, 256)), 0.0)
            kron[k, 16 * q:16 * q + 16] = blk.astype(BF16)
        return 0

    lax.fori_loop(0, GROUP, build, 0)

    def rest(ks, ts):
        res = None
        for k in ks:
            zs = []
            for t in ts:
                blk = u[:, k, 16 * t:16 * t + 16].reshape(256, BOND)
                zs.append(jnp.dot(kron[k], blk, preferred_element_type=F32).astype(BF16))
            zk = zs[0] if len(zs) == 1 else jnp.concatenate(zs, axis=0)
            o = jnp.dot(zk, rall[k], preferred_element_type=F32)
            res = o if res is None else res + o
        for i, t in enumerate(ts):
            acc[t] += res[256 * i:256 * i + 256].reshape(Y, QY, 16, BOND)

    slab = (c, 1 - c)

    def handover():
        return pltpu.make_async_remote_copy(acc.at[1 - c], accin, x_send.at[0], x_recv.at[0],
                                            device_id=sib, device_id_type=MESH)

    def mine_(t, *i):
        return acc[(c, *i)] if t == 0 else accin[i]

    def ycopy(t, d):
        yt = up(y, d, Y)
        return pltpu.make_async_remote_copy(acc.at[c, yt] if t == 0 else accin.at[yt], yrecv.at[t, d - 1], y_send.at[t, d - 1], y_recv.at[t, d - 1],
                                            device_id=dev(z, yt, x, c), device_id_type=MESH)

    def ystart(t):
        for d in range(1, Y):
            ycopy(t, d).start()

    def adot(t, slot):
        part = jnp.zeros((8, BOND), F32)
        for q in range(PAIR):
            prod = mine_(t, q // QY, q % QY) * v[slot, q, x, slab[t]]
            part = part + prod[:8] + prod[8:]
        return part

    def acopy(which, par, d):
        if d < PLANE:
            ref, to = pm.at[which, place], (PLANE * z + lax.rem(place + d, PLANE),)
            sems = p_send.at[which, d - 1], p_recv.at[which, d - 1]
        else:
            d = d - PLANE + 1
            ref, to = zm.at[par, which, z], dev(up(z, d, Z), y, x, c)
            sems = a_send.at[par, which, d - 1], a_recv.at[par, which, d - 1]
        return pltpu.make_async_remote_copy(ref, ref, *sems, device_id=to, device_id_type=MESH)

    IN_PLANE, IN_Z = range(1, PLANE), range(PLANE, PLANE + Z - 1)

    def plane_start(which, par, part):
        pm[which, place] = jnp.sum(part[:, :128] + part[:, 128:], axis=0, keepdims=True)
        for d in IN_PLANE:
            acopy(which, par, d).start()

    def plane_done(which, par):
        for d in IN_PLANE:
            acopy(which, par, d).wait_recv()
        sums = [pm[which, i] for i in range(PLANE)]
        while len(sums) > 1:
            sums = [a + b for a, b in zip(sums[::2], sums[1::2])]
        zm[par, which, z] = sums[0]
        for d in IN_Z:
            acopy(which, par, d).start()

    def scalar(which, par):
        for d in IN_Z:
            acopy(which, par, d).wait_recv()
        sums = [zm[par, which, i] for i in range(Z)]
        while len(sums) > 1:
            sums = [a + b for a, b in zip(sums[::2], sums[1::2])]
        return jnp.sum(sums[0], axis=1, keepdims=True) / COUNT

    def abegin(par, slot):
        plane_start(0, par, adot(0, slot) + adot(1, slot))

    def on(core, *acts):
        @pl.when(c == core)
        def _():
            for act in acts:
                act()

    def take():
        handover().wait_recv()
        ystart(1)

    def blocks():
        acc[...] = jnp.zeros_like(acc)

        rest(list(range(GROUP)), [0])
        on(1, lambda: handover().start())
        on(0, lambda: ystart(0))
        rest(list(range(UNROLL)), [1])
        on(0, take)
        rest(list(range(UNROLL, GROUP)), [1])
        on(1, lambda: ystart(0))
        on(0, lambda: handover().start())

    def tail(j, beta_prev, last):
        st = Span()
        par = lax.rem(j, 2)
        sent = []
        hz = lax.rem(z, 2)
        qz = QY * y + z // 2

        def ydone(t):
            for d in range(1, Y):
                ycopy(t, d).wait_recv()
            ysum = mine_(t, y) + yrecv[t, 0] + yrecv[t, 1] + yrecv[t, 2]
            zsend[t] = ysum.reshape(Z, 8, BOND)
            zc = []
            for d in range(1, Z):
                zt = up(z, d, Z)
                zc.append(send(zsend.at[t, zt], zrecv.at[t, d - 1], z_send.at[t, d - 1], z_recv.at[t, d - 1], dev(zt, y, x, c)))
            sent.extend(zc)
            return zc

        def zdone(t, zc):
            for copy in zc:
                copy.wait_recv()
            zsum = zsend[t, z]
            for d in range(Z - 1):
                zsum = zsum + zrecv[t, d]
            s[par, qz, x, slab[t], hz] = zsum
            ch = s.at[par, qz, x, slab[t], hz]
            gz = [send(ch, ch, gz_send.at[par, t, d - 1], gz_recv.at[par, t, d - 1], dev(up(z, d, Z), y, x, c))
                  for d in range(1, Z)]
            sent.extend(gz)
            return gz

        slot = [0]

        def piece(part, i, k, q):
            t, h = part
            xx, yy = (k, i) if h == 0 else (i, k)
            return s.at[par, pl.ds(QY * yy + q[0], q[1]), xx, slab[t], :, :, pl.ds(128 * h, 128)]

        qa, q0, q1 = (0, QY), (0, QY // 2), (QY // 2, QY // 2)

        def go(ref, to):
            i = slot[0]
            slot[0] += 1
            copy = send(ref, ref, gr_send.at[par, i], gr_recv.at[par, i], to)
            sent.append(copy)
            return copy

        ax = [((y, yp, ym, y2, typ, tym), (x, xp, xm, x2, txp, txm)),
              ((x, xp, xm, x2, txp, txm), (y, yp, ym, y2, typ, tym))]
        far = [dev(z, y2, x, c), dev(z, y, x2, c)]
        one, two, rel2 = {}, {}, {}

        def second(part, i, tag):
            (_, (w, _, _, _, tp, tm)) = ax[part[1]]
            two[part, tag] = [go(piece(part, i, w, qa), tp), go(piece(part, i, w, qa), tm), i]
            if tag in DIRECT2[part[0]]:
                two[part, tag].append(go(piece(part, i, w, qa), far[1 - part[1]]))

        def relay2(part, tag):
            (_, (w, wp, wm, _, tp, tm)) = ax[part[1]]
            cp, cm, i, *direct = two[part, tag]
            cp.wait_recv()
            if direct:
                cm.wait_recv()
                rel2[part, tag] = direct
                return
            a = go(piece(part, i, wm, q0), tp)
            cm.wait_recv()
            b = go(piece(part, i, wp, q1), tm)
            rel2[part, tag] = [a, b]

        def open_(t, gz):
            for copy in gz:
                copy.wait_recv()
            for h in (0, 1):
                ((w, _, _, _, tp, tm), (k, *_)) = ax[h]
                one[t, h] = [go(piece((t, h), w, k, qa), to) for to in (tp, tm, far[h])]
            for h in (0, 1):
                second((t, h), ax[h][0][0], "own")

        def near(t):
            for h in (0, 1):
                ((w, wp, wm, _, tp, tm), (k, *_)) = ax[h]
                one[t, h][0].wait_recv()
                second((t, h), wm, "m")
                one[t, h][1].wait_recv()
                second((t, h), wp, "p")

        def distant(t):
            for h in (0, 1):
                one[t, h][2].wait_recv()
                second((t, h), ax[h][0][3], "2")

        def relays(t, tag):
            for h in (0, 1):
                relay2((t, h), tag)

        st("take")
        on(1, take)
        abegin(par, par)
        st("rs0")
        z0 = ydone(0)
        st("rs1")
        z1 = ydone(1)
        st("z0")
        g0 = zdone(0, z0)
        plane_done(0, par)
        st("z1")
        g1 = zdone(1, z1)
        st("g0")
        open_(0, g0)
        st("g1")
        open_(1, g1)
        cur, prev = lax.rem(j, 2), lax.rem(j + 1, 2)
        alpha = scalar(0, par)
        part = jnp.zeros((8, BOND), F32)
        rows8 = pl.ds(pl.multiple_of(8 * hz, 8), 8)
        for t in (0, 1):
            w = (s[par, qz, x, slab[t], hz] - alpha * v[cur, qz, x, slab[t], rows8]
                 - beta_prev * v[prev, qz, x, slab[t], rows8])
            part = part + w * w
        plane_start(1, par, part)
        st("n0")
        near(0)
        st("n1")
        near(1)
        st("o0")
        relays(0, "own")
        distant(0)
        st("o1")
        relays(1, "own")
        distant(1)
        plane_done(1, par)
        st("ag3")
        for tag in ("m", "p", "2"):
            for t in (0, 1):
                relays(t, tag)
        for t in (0, 1):
            for tag in ("own", "m", "p", "2"):
                for h in (0, 1):
                    for copy in rel2[(t, h), tag]:
                        copy.wait_recv()
        st("beta")
        beta = jnp.sqrt(scalar(1, par))
        inv = 1.0 / beta
        for t in (0, 1):
            for d in range(1, Y):
                ycopy(t, d).wait_send()
        handover().wait_send()
        st("v3")

        def value(i):
            return (sload(par, i) - alpha * vload(cur, i) - beta_prev * vload(prev, i)) * inv

        copies = finish(prev, value, j + 1)
        scalars[0, j] = alpha[0, 0]
        scalars[1, j] = beta[0, 0]
        for copy in sent:
            copy.wait_send()
        for which in (0, 1):
            for d in (*IN_PLANE, *IN_Z):
                acopy(which, par, d).wait_send()
        if last:
            settle(copies, 0)
        else:
            st("stage1")
            first(copies)
            st("blocks")
            blocks()
        st("")
        return beta

    sp("first")
    first(begun)
    acc[...] = jnp.zeros_like(acc)
    msib = C * x + 1 - c
    mm, mp, m2 = C * xm + c, C * xp + c, C * x2 + c
    sm, sq_, s2 = C * xm + 1 - c, C * xp + 1 - c, C * x2 + 1 - c
    base = 3 * PART

    def terms(m, h):
        return [OWN * m + PT * h + i for i in range(PT)]

    def arrive(copies, m, h, i, on=()):
        for copy in copies:
            copy.wait_recv()
        far_ = []
        for slot_, to, kinds in on:
            far_ += qsend(rall, OWN * m + PT * h, m, h, slot_, to, kinds)
        mirror(m, h)
        return far_, rsend(rpart(m, h), rpart(m, h), i, 0, sib)

    sp("R0")
    far0, a0 = arrive(from_xm[0], mm, 0, base + 3, [(base + 0, txp, (0, 1))])
    far2, b2 = arrive(from_xp[2], mp, 2, base + 8, [(base + 2, txm, (0, 1))])
    for h in range(PART):
        from_sib[h].wait_recv()
    rest([k for h in range(PART) for m in (mem, msib) for k in terms(m, h)], (0, 1))
    sp("R1")
    far1b, a1 = arrive(from_xm[1], mm, 1, base + 4, [(base + 1, txp, (1,))])
    far1a, b1 = arrive(from_xp[1], mp, 1, base + 7, [(base + 1, txm, (0,))])
    a0.wait_recv()
    b2.wait_recv()
    rest(terms(mm, 0) + terms(sm, 0) + terms(mp, 2) + terms(sq_, 2), (0, 1))
    sp("R2")
    _, a2 = arrive(from_xm[2], mm, 2, base + 5)
    _, b0 = arrive(from_xp[0], mp, 0, base + 6)
    a1.wait_recv()
    b1.wait_recv()
    rest(terms(mm, 1) + terms(sm, 1) + terms(mp, 1) + terms(sq_, 1), (0, 1))
    sp("R3")
    _, f0 = arrive(far0, m2, 0, base + 9)
    _, f2 = arrive(far2, m2, 2, base + 11)
    a2.wait_recv()
    b0.wait_recv()
    rest(terms(mm, 2) + terms(sm, 2) + terms(mp, 0) + terms(sq_, 0), (0, 1))
    sp("R4")
    _, f1 = arrive(far1a + far1b, m2, 1, base + 10)
    f0.wait_recv()
    f2.wait_recv()
    rest(terms(m2, 0) + terms(s2, 0) + terms(m2, 2) + terms(s2, 2), (0, 1))
    sp("R5")
    f1.wait_recv()
    rest(terms(m2, 1) + terms(s2, 1), (0, 1))
    for copy in early + pend:
        copy.wait_send()
    sp("")

    handover().start()
    ystart(0)
    on(0, take)

    def step(j, beta_prev):
        return tail(j, beta_prev, False)

    tail(STEPS - 1, lax.fori_loop(0, STEPS - 1, step, jnp.zeros((1, 1), F32)), True)
    mine = lax.rem(me // 16, 2) == c
    out[...] = jnp.where(mine, rown[...], rrecv[...])


def solution(mesh):
    def local_run(psi_init, left_env, op_pair, right_env):
        dma = pltpu.SemaphoreType.DMA
        any_ = pl.BlockSpec(memory_space=pl.ANY)
        rows = pltpu.VMEM((STEPS + 1, PAIR, BOND), F32)
        out, scalars = pl.pallas_call(
            kernel,
            out_shape=(jax.ShapeDtypeStruct((STEPS + 1, PAIR, BOND), F32),
                       jax.ShapeDtypeStruct((2, STEPS), F32)),
            in_specs=[any_] * 4,
            out_specs=(pl.BlockSpec(memory_space=pltpu.VMEM),
                       pl.BlockSpec(memory_space=pltpu.SMEM)),
            scratch_shapes=[
                pltpu.VMEM((GROUP, SLAB, BOND), BF16),
                pltpu.VMEM((GROUP, PAIR, PAIR), BF16),
                pltpu.VMEM((GROUP, PAIR, 256), F32),
                pltpu.VMEM((GROUP, BOND, BOND), BF16),
                pltpu.VMEM((GROUP, 256, 256), BF16),
                pltpu.VMEM((PAIR, GROUP, SLAB, BOND), BF16),
                pltpu.VMEM((PAIR, X, C, 2, 16, BOND), BF16),
                pltpu.VMEM((2, PAIR, X, C, 16, BOND), F32),
                pltpu.VMEM((2, PAIR, X, C, 2, 8, BOND), F32),
                pltpu.VMEM((2, Y, QY, 16, BOND), F32),
                pltpu.VMEM((Y, QY, 16, BOND), F32),
                pltpu.VMEM((2, Y - 1, QY, 16, BOND), F32),
                pltpu.VMEM((2, Z, 8, BOND), F32),
                pltpu.VMEM((2, Z - 1, 8, BOND), F32),
                pltpu.VMEM((8, 128), F32),
                pltpu.VMEM((8, 128), F32),
                pltpu.VMEM((2, PLANE, 1, 128), F32),
                pltpu.VMEM((2, 2, Z, 1, 128), F32),
                rows, rows, rows,
                dma((20,)), dma((2, 7)), dma((2, 7)),
                dma((21, 2)), dma((21, 2)),
                dma((1,)), dma((1,)),
                dma((2, 3)), dma((2, 3)), dma((2, 7)), dma((2, 7)),
                dma((2, 2, 7)), dma((2, 2, 7)),
                dma((2, 80)), dma((2, 80)),
                dma((1,)), dma((1,)),
                dma((2, PLANE - 1)), dma((2, PLANE - 1)), dma((2, 2, Z - 1)), dma((2, 2, Z - 1)),
                dma((4,)), dma((4,)),
                dma((1,)), dma((1,)),
            ],
            compiler_params=pltpu.CompilerParams(
                collective_id=0, has_side_effects=True, vmem_limit_bytes=66 * 1000 * 1000),
        )(psi_init.reshape(X, C, 2, 16, 4, 4, BOND), left_env, op_pair, right_env)
        return out.reshape(STEPS + 1, 1, 4, 4, BOND), scalars[0], scalars[1]

    return jax.shard_map(local_run, mesh=mesh, in_specs=(P(), P("terms"), P("terms"), P("terms")),
                         out_specs=(P(None, "terms"), P(), P()), check_vma=False)
```
